256 devices in a mesh: parts: 2 (over x_hi), context: 16 (over z, core), tensor: 8 (over y, x_lo).
Axes of the slice: x: 4 (x_hi: 2, x_lo: 2; x = x_hi * 2 + x_lo), y: 4, z: 8, core: 2. Of those that a mesh axis runs over, the one named last changes fastest.
Arguments:
- queries: bfloat16 [8192, 8192], P(('parts', 'context'), 'tensor'), parts along dimension 0, may hold values from -13 to 13
- keys: bfloat16 [8192, 1024], P(('parts', 'context'), 'tensor'), parts along dimension 0, may hold values from -5.2 to 5.2
- values: bfloat16 [8192, 1024], P(('parts', 'context'), 'tensor'), parts along dimension 0, may hold values from -6 to 6
- out_weight: bfloat16 [8192, 4096], P('tensor'), may hold values from -0.1875 to 0.1875
Outputs:
- mixed: bfloat16 [8192, 4096], P(('parts', 'context'), 'tensor'), parts along dimension 0
The draws below stay inside these ranges and needn't reach their ends.
There are 2 independent parts, one for each index of `parts`. The reference program is written for one: setup_inputs(seed, part) draws one part's arguments, and reference() takes and returns one part's arrays. A program takes and returns all parts, laid end to end along the dimension named above; an argument that names none is the same for every part. Nothing has to cross between parts.
All inputs are finite; a program needn't handle non-finite values.
Results may differ from the reference program's by a relative error of at most 0.015.
Values may be sent and summed in bfloat16 or wider, within the bound.
No kernel may reach another device: no remote copies, remote signals or barrier semaphores. Data moves between devices by JAX's collectives and lax.ppermute only.
A program may use at most 64 MiB of HBM per device.

```python
import jax
import jax.numpy as jnp
from jax import lax

D = 4096
HD = 128
HQ = 64
KVH = 8
TOKENS = 4096
N_TENSOR = 8


def draw_common(key):
    key_base = jnp.clip(jax.random.normal(jax.random.fold_in(key, 21), (TOKENS, KVH * HD), jnp.float32), -4.0, 4.0)
    query_base = jnp.clip(2.5 * jax.random.normal(jax.random.fold_in(key, 22), (TOKENS, HQ * HD), jnp.float32), -10.0, 10.0)
    return (query_base, key_base)


def draw_queries(key, part):
    query_base, key_base = draw_common(key)
    return query_base.astype(jnp.bfloat16)


def draw_keys(key, part):
    query_base, key_base = draw_common(key)
    return key_base.astype(jnp.bfloat16)


def levels(own_key, shape, shards, low, top_value):
    loudness, own = 1.0, jax.random.fold_in(own_key, 6)
    for position, shards_of in shards:
        steps = jnp.exp(jax.random.uniform(jax.random.fold_in(own, position), (shards_of,), jnp.float32, low / len(shards), top_value / len(shards)))
        loudness = loudness * jnp.repeat(steps, shape[position] // shards_of).reshape([-1 if axis == position else 1 for axis in range(len(shape))])
    return loudness


def gaussian(own_key, dims, scale, bound, split=(), kind=jnp.bfloat16):
    array = jax.random.normal(own_key, dims, jnp.float32) * scale
    if len(split) > 0:
        array = levels(own_key, dims, split, -0.22, 0.18) * array
    return jnp.clip(array, min=-bound, max=bound).astype(kind)


def setup_inputs(seed: int = 0, part: int = 0) -> dict:
    streams_of = jax.random.split(jax.random.key(seed), 5)
    part_splits = jax.random.split(jax.random.fold_in(streams_of[4], part), 5)
    return {
        "queries": draw_queries(jax.random.fold_in(jax.random.fold_in(streams_of[4], part), 71), part),
        "keys": draw_keys(jax.random.fold_in(jax.random.fold_in(streams_of[4], part), 71), part),
        "values": gaussian(part_splits[2], (TOKENS, KVH * HD), 1.0, 6.0, ((0, 16), (1, 8))),
        "out_weight": gaussian(streams_of[3], (HQ * HD, D), (HQ * HD // 8) ** -0.5, 0.1875, ((0, 8),)),
    }


def reference(queries, keys, values, out_weight):
    tok_count = queries.shape[0]
    group_size = HQ // KVH
    query_heads = queries.reshape(tok_count, HQ, HD).transpose(1, 0, 2)
    key_heads = keys.reshape(tok_count, KVH, HD).transpose(1, 0, 2)
    value_heads = values.reshape(tok_count, KVH, HD).transpose(1, 0, 2)
    positions = jnp.arange(tok_count, dtype=jnp.int32)
    visible = positions[None, :] <= positions[:, None]

    def one_head(head_idx):
        kv_idx = head_idx // group_size
        query_mat = query_heads[head_idx]
        key_mat = key_heads[kv_idx]
        value_mat = value_heads[kv_idx]
        scores = jnp.dot(query_mat, key_mat.T, preferred_element_type=jnp.float32) * (HD ** -0.5)
        scores = jnp.where(visible, scores, -jnp.inf)
        top_val = jnp.max(scores, axis=1, keepdims=True)
        expo = jnp.exp(scores - top_val)
        totals = jnp.sum(expo, axis=1, keepdims=True)
        mixed_head = jnp.dot(expo.astype(jnp.bfloat16), value_mat, preferred_element_type=jnp.float32) / totals
        return mixed_head.astype(jnp.bfloat16)

    head_outs = lax.map(one_head, jnp.arange(HQ, dtype=jnp.int32))
    attended = head_outs.transpose(1, 0, 2).reshape(tok_count, HQ * HD)
    width_share = HQ * HD // N_TENSOR
    summed = jnp.zeros((tok_count, D), jnp.float32)
    for group_idx in range(N_TENSOR):
        cols = attended[:, group_idx * width_share:(group_idx + 1) * width_share]
        rows_part = out_weight[group_idx * width_share:(group_idx + 1) * width_share]
        partial_value = jnp.dot(cols, rows_part, preferred_element_type=jnp.float32)
        rounded = lax.optimization_barrier(partial_value.astype(jnp.bfloat16))
        summed = summed + rounded.astype(jnp.float32)
    return summed.astype(jnp.bfloat16)
```

```python
import jax
import jax.numpy as jnp
from jax import lax
from jax.experimental import pallas as pl
from jax.experimental.pallas import tpu as pltpu
from jax.sharding import Mesh
from jax.sharding import PartitionSpec as P

HD = 128
LOG2E = 1.4426950408889634
SCALE = LOG2E * HD ** (-0.5)
PARTS_CONTEXT = ("parts", "z", "core")
VMEM = pl.BlockSpec(memory_space=pltpu.VMEM)
SMEM = pl.BlockSpec(memory_space=pltpu.SMEM)
LIMIT = 20 * 2**20


def params():
    return pltpu.CompilerParams(vmem_limit_bytes=LIMIT)


def cost(keys, rows, heads):
    return pl.CostEstimate(
        flops=4 * keys * rows * heads * HD,
        bytes_accessed=4 * keys * HD + 4 * heads * rows * HD,
        transcendentals=keys * rows * heads,
    )


def absorb(blocks, state, first=False, diag=False):
    q_ref, top_ref, sum_ref, acc_ref = state
    heads = q_ref.shape[0]
    join = (lambda parts: parts[0] if len(parts) == 1 else jnp.concatenate(parts, 0))
    keys = join([b[0] for b in blocks])
    values_t = join([b[1] for b in blocks]).T
    span = keys.shape[0]
    values_t = jnp.concatenate([values_t, jnp.ones((16, span), jnp.bfloat16)], 0)
    if diag:
        shape = (span, q_ref.shape[2])
        keep = lax.broadcasted_iota(jnp.int32, shape, 0) <= lax.broadcasted_iota(jnp.int32, shape, 1)

    def scores_of(h):
        return jnp.dot(keys, q_ref[h], preferred_element_type=jnp.float32) * SCALE

    ahead = scores_of(0)
    for h in range(heads):
        scores = ahead
        if h + 1 < heads:
            ahead = scores_of(h + 1)
        if diag:
            scores = jnp.where(keep, scores, -jnp.inf)
        top = jnp.max(scores, axis=0, keepdims=True)
        if not first:
            old = top_ref[h]
            top = jnp.maximum(old, top)
            shrink = jnp.exp2(old - top)
        weights = jnp.exp2(scores - top).astype(jnp.bfloat16)
        both = jnp.dot(values_t, weights, preferred_element_type=jnp.float32)
        acc, total = both[:HD], both[HD : HD + 1]
        top_ref[h] = top
        if first:
            sum_ref[h] = total
            acc_ref[h] = acc
        else:
            sum_ref[h] = sum_ref[h] * shrink + total
            acc_ref[h] = acc_ref[h] * shrink + acc


def open_state(where, queries, own, other):
    rows, width = queries.shape
    heads = width // HD

    def kernel(where_ref, queries_ref, own_ref, other_ref, *state):
        for h in range(heads):
            state[0][h] = queries_ref[:, h * HD : (h + 1) * HD].T
        absorb([own_ref], state, first=True, diag=True)

        @pl.when(where_ref[1] == 1)
        def _():
            absorb([other_ref], state)

    return pl.pallas_call(
        kernel,
        out_shape=(
            jax.ShapeDtypeStruct((heads, HD, rows), jnp.bfloat16),
            jax.ShapeDtypeStruct((heads, 1, rows), jnp.float32),
            jax.ShapeDtypeStruct((heads, 1, rows), jnp.float32),
            jax.ShapeDtypeStruct((heads, HD, rows), jnp.float32),
        ),
        in_specs=[SMEM, VMEM, VMEM, VMEM],
        out_specs=(VMEM,) * 4,
        compiler_params=params(),
        cost_estimate=cost(2 * rows, rows, heads),
        name="open_state",
    )(where, queries, own, other)


def fold(where, state, ahead, behind, step):
    n_ahead = len(ahead)

    def kernel(where_ref, *refs):
        block_refs, state_in, state_out = refs[: n_ahead + len(behind)], refs[-7:-3], refs[-3:]
        z = where_ref[0]
        size = where_ref[2]
        live = (state_in[0],) + tuple(state_out)
        for src, dst in zip(state_in[1:], state_out):
            dst[...] = src[...]
        if behind:

            @pl.when(z + step >= size)
            def _():
                absorb(block_refs, live)

            @pl.when((z + step < size) & (z >= step))
            def _():
                absorb(block_refs[:n_ahead], live)
        else:

            @pl.when(z >= step)
            def _():
                absorb(block_refs, live)

    q, top, total, acc = state
    blocks = tuple(ahead) + tuple(behind)
    heads, _, rows = q.shape
    out = pl.pallas_call(
        kernel,
        out_shape=tuple(jax.ShapeDtypeStruct(a.shape, a.dtype) for a in state[1:]),
        in_specs=[SMEM] + [VMEM] * (len(blocks) + 4),
        out_specs=(VMEM,) * 3,
        compiler_params=params(),
        cost_estimate=cost(len(blocks) * blocks[0].shape[1], rows, heads),
        name=f"fold_{step}",
    )(where, *blocks, *state)
    return (q,) + tuple(out)


def close(where, state, ahead, step, out_weight, pieces):
    q, _, _, acc = state
    heads, _, rows = q.shape
    width = out_weight.shape[1] // pieces

    def kernel(where_ref, *refs):
        block_refs = refs[: len(ahead)]
        state_in = refs[len(ahead) : len(ahead) + 4]
        weight_ref, out_ref, top_ref, sum_ref, acc_ref, att_ref = refs[len(ahead) + 4 :]
        live = (state_in[0], top_ref, sum_ref, acc_ref)

        @pl.when(pl.program_id(0) == 0)
        def _():
            for src, dst in zip(state_in[1:], live[1:]):
                dst[...] = src[...]

            @pl.when(where_ref[0] >= step)
            def _():
                absorb(block_refs, live)

            for h in range(heads):
                att_ref[:, h * HD : (h + 1) * HD] = (acc_ref[h] / sum_ref[h]).T.astype(jnp.bfloat16)

        out_ref[0] = jnp.dot(att_ref[...], weight_ref[...], preferred_element_type=jnp.float32).astype(jnp.bfloat16)

    fixed = lambda a: pl.BlockSpec(a.shape, lambda j, n=a.ndim: (0,) * n)
    return pl.pallas_call(
        kernel,
        grid=(pieces,),
        out_shape=jax.ShapeDtypeStruct((pieces, rows, width), jnp.bfloat16),
        in_specs=[SMEM]
        + [fixed(a) for a in (*ahead, *state)]
        + [pl.BlockSpec((heads * HD, width), lambda j: (0, j))],
        out_specs=pl.BlockSpec((1, rows, width), lambda j: (j, 0, 0)),
        scratch_shapes=[
            pltpu.VMEM((heads, 1, rows), jnp.float32),
            pltpu.VMEM((heads, 1, rows), jnp.float32),
            pltpu.VMEM((heads, HD, rows), jnp.float32),
            pltpu.VMEM((rows, heads * HD), jnp.bfloat16),
        ],
        compiler_params=params(),
        cost_estimate=cost(2 * rows, rows, heads),
        name="close",
    )(where, *ahead, *state, out_weight)


def body(queries, keys, values, out_weight):
    chips = lax.axis_size("z")
    z = lax.axis_index("z")
    core = lax.axis_index("core")
    where = jnp.stack([z, core, jnp.int32(chips)]).astype(jnp.int32)
    up = [(i, (i + 1) % chips) for i in range(chips)]
    down = [(i, (i - 1) % chips) for i in range(chips)]
    swap = lambda a: lax.ppermute(a, "core", [(0, 1), (1, 0)])
    own = jnp.stack([keys, values])
    half = chips // 2
    ahead, behind = [own], [own]
    for k in range(1, half + 1):
        ahead.append(lax.ppermute(ahead[-1], "z", up))
        if k < half:
            behind.append(lax.ppermute(behind[-1], "z", down))
    state = open_state(where, queries, own, swap(own))
    for k in range(1, half):
        state = fold(where, state, (ahead[k], swap(ahead[k])), (behind[k], swap(behind[k])), k)
    pieces = lax.axis_size("tensor")
    terms = close(where, state, (ahead[half], swap(ahead[half])), half, out_weight, pieces)
    got = lax.all_to_all(terms, "tensor", 0, 0, tiled=True)
    return jnp.sum(got.astype(jnp.float32), axis=0).astype(jnp.bfloat16)


def solution(mesh):
    finer = Mesh(
        mesh.devices.reshape(mesh.shape["parts"], mesh.shape["context"] // 2, 2, mesh.shape["tensor"]),
        ("parts", "z", "core", "tensor"),
    )
    in_specs = (
        P(PARTS_CONTEXT, "tensor"),
        P(PARTS_CONTEXT, "tensor"),
        P(PARTS_CONTEXT, "tensor"),
        P("tensor", None),
    )
    out_specs = P(PARTS_CONTEXT, "tensor")
    return jax.shard_map(body, mesh=finer, in_specs=in_specs, out_specs=out_specs, check_vma=False)
```

```python
import jax
import jax.numpy as jnp
from jax import lax
from jax.experimental import pallas as pl
from jax.experimental.pallas import tpu as pltpu
from jax.sharding import Mesh
from jax.sharding import PartitionSpec as P

HD = 128
LOWEST = -1e30
LOG2E = 1.4426950408889634
SCALE = LOG2E * HD ** (-0.5)
PARTS_CONTEXT = ("parts", "z", "core")
VMEM = pl.BlockSpec(memory_space=pltpu.VMEM)
SMEM = pl.BlockSpec(memory_space=pltpu.SMEM)
LIMIT = 20 * 2**20


def params():
    return pltpu.CompilerParams(vmem_limit_bytes=LIMIT)


def cost(keys, rows, heads):
    return pl.CostEstimate(
        flops=4 * keys * rows * heads * HD,
        bytes_accessed=4 * keys * HD + 4 * heads * rows * HD,
        transcendentals=keys * rows * heads,
    )


def absorb(blocks, state, first=False, diag=False):
    q_ref, top_ref, sum_ref, acc_ref = state
    heads = top_ref.shape[0]
    merge = (lambda parts: parts[0] if len(parts) == 1 else jnp.concatenate(parts, 0))
    keys = merge([b[0] for b in blocks])
    values_t = merge([b[1] for b in blocks]).T
    span = keys.shape[0]
    values_t = jnp.concatenate([values_t, jnp.ones((16, span), jnp.bfloat16)], 0)
    if diag:
        shape = (span, q_ref.shape[2])
        keep = lax.broadcasted_iota(jnp.int32, shape, 0) <= lax.broadcasted_iota(jnp.int32, shape, 1)

    def scores_of(h):
        return jnp.dot(keys, q_ref[h], preferred_element_type=jnp.float32) * SCALE

    ahead = scores_of(0)
    for h in range(heads):
        scores = ahead
        if h + 1 < heads:
            ahead = scores_of(h + 1)
        if diag:
            scores = jnp.where(keep, scores, -jnp.inf)
        top = jnp.max(scores, axis=0, keepdims=True)
        if not first:
            old = top_ref[h]
            top = jnp.maximum(old, top)
            shrink = jnp.exp2(old - top)
        weights = jnp.exp2(scores - top).astype(jnp.bfloat16)
        both = jnp.dot(values_t, weights, preferred_element_type=jnp.float32)
        acc, total = both[:HD], both[HD : HD + 1]
        top_ref[h] = top
        if first:
            sum_ref[h] = total
            acc_ref[h] = acc
        else:
            sum_ref[h] = sum_ref[h] * shrink + total
            acc_ref[h] = acc_ref[h] * shrink + acc


def sds(shape, dtype):
    return jax.ShapeDtypeStruct(shape, dtype)


def open_state(where, queries, others, own):
    rows, width = queries.shape
    heads = width // HD

    def kernel(where_ref, queries_ref, others_ref, own_ref, *state):
        for h in range(heads):
            state[0][h] = queries_ref[:, h * HD : (h + 1) * HD].T
            state[0][heads + h] = others_ref[:, h * HD : (h + 1) * HD].T
        absorb([own_ref], [r.at[:heads] for r in state], first=True, diag=True)
        rest = [r.at[heads:] for r in state]

        @pl.when(where_ref[1] == 0)
        def _():
            absorb([own_ref], rest, first=True)

        @pl.when(where_ref[1] != 0)
        def _():
            rest[1][...] = jnp.full(rest[1].shape, LOWEST, jnp.float32)
            rest[2][...] = jnp.zeros(rest[2].shape, jnp.float32)
            rest[3][...] = jnp.zeros(rest[3].shape, jnp.float32)

    return pl.pallas_call(
        kernel,
        out_shape=(
            sds((2 * heads, HD, rows), jnp.bfloat16),
            sds((2 * heads, 1, rows), jnp.float32),
            sds((2 * heads, 1, rows), jnp.float32),
            sds((2 * heads, HD, rows), jnp.float32),
        ),
        in_specs=[SMEM, VMEM, VMEM, VMEM],
        out_specs=(VMEM,) * 4,
        compiler_params=params(),
        cost_estimate=cost(rows, rows, 2 * heads),
        name="open_state",
    )(where, queries, others, own)


def fold(where, state, ahead, behind, step, parting):
    def kernel(where_ref, ahead_ref, behind_ref, *refs):
        live = refs[:4]
        z = where_ref[0]
        size = where_ref[2]

        @pl.when(z + step >= size)
        def _():
            absorb([ahead_ref, behind_ref], live)

        @pl.when((z + step < size) & (z >= step))
        def _():
            absorb([ahead_ref], live)

        if parting:
            out_ref, stat_ref = refs[-2:]
            heads = live[0].shape[0] // 2
            for h in range(heads):
                total = live[2][heads + h]
                scale = jnp.where(total > 0, 1.0 / jnp.where(total > 0, total, 1.0), 0.0)
                out_ref[h] = (live[3][heads + h] * scale).astype(jnp.bfloat16)
                stat_ref[0, h] = live[1][heads + h]
                stat_ref[1, h] = total

    heads, _, rows = state[0].shape
    extra = (sds((heads // 2, HD, rows), jnp.bfloat16), sds((2, heads // 2, 1, rows), jnp.float32)) if parting else ()
    out = pl.pallas_call(
        kernel,
        out_shape=tuple(sds(a.shape, a.dtype) for a in state) + extra,
        in_specs=[SMEM] + [VMEM] * 6,
        out_specs=(VMEM,) * (4 + len(extra)),
        input_output_aliases={3 + i: i for i in range(4)},
        compiler_params=params(),
        cost_estimate=cost(2 * ahead.shape[1], rows, heads),
    )(where, ahead, behind, *state)
    return (out[:4], out[4:]) if parting else out


def join(where, state, parted, stats, ahead, step):
    heads, _, rows = parted.shape

    def kernel(where_ref, parted_ref, stats_ref, ahead_ref, *refs):
        state_in, state_out = refs[:4], refs[4:]
        live = (state_in[0].at[:heads],) + tuple(state_out)
        for h in range(heads):
            old, theirs = state_in[1][h], stats_ref[0, h]
            top = jnp.maximum(old, theirs)
            mine = jnp.exp2(old - top)
            part = jnp.exp2(theirs - top) * stats_ref[1, h]
            state_out[0][h] = top
            state_out[1][h] = state_in[2][h] * mine + part
            state_out[2][h] = state_in[3][h] * mine + parted_ref[h].astype(jnp.float32) * part

        @pl.when(where_ref[0] >= step)
        def _():
            absorb([ahead_ref], live)

    return pl.pallas_call(
        kernel,
        out_shape=tuple(sds((heads, *a.shape[1:]), a.dtype) for a in state[1:]),
        in_specs=[SMEM] + [VMEM] * 7,
        out_specs=(VMEM,) * 3,
        compiler_params=params(),
        cost_estimate=cost(ahead.shape[1], rows, heads),
        name="join",
    )(where, parted, stats, ahead, *state)


def close(where, state, ahead, step, out_weight, pieces):
    heads, _, rows = state[3].shape
    width = out_weight.shape[1] // pieces

    def kernel(where_ref, ahead_ref, q_ref, top_ref, sum_ref, acc_ref, weight_ref, out_ref, live_top, live_sum, live_acc, att_ref):
        live = (q_ref.at[:heads], live_top, live_sum, live_acc)

        @pl.when(pl.program_id(0) == 0)
        def _():
            for src, dst in zip((top_ref, sum_ref, acc_ref), live[1:]):
                dst[...] = src[...]

            @pl.when(where_ref[0] >= step)
            def _():
                absorb([ahead_ref], live)

            for h in range(heads):
                att_ref[:, h * HD : (h + 1) * HD] = (live_acc[h] / live_sum[h]).T.astype(jnp.bfloat16)

        out_ref[0] = jnp.dot(att_ref[...], weight_ref[...], preferred_element_type=jnp.float32).astype(jnp.bfloat16)

    fixed = lambda a: pl.BlockSpec(a.shape, lambda j, n=a.ndim: (0,) * n)
    return pl.pallas_call(
        kernel,
        grid=(pieces,),
        out_shape=sds((pieces, rows, width), jnp.bfloat16),
        in_specs=[SMEM, fixed(ahead)]
        + [fixed(a) for a in state]
        + [pl.BlockSpec((heads * HD, width), lambda j: (0, j))],
        out_specs=pl.BlockSpec((1, rows, width), lambda j: (j, 0, 0)),
        scratch_shapes=[
            pltpu.VMEM((heads, 1, rows), jnp.float32),
            pltpu.VMEM((heads, 1, rows), jnp.float32),
            pltpu.VMEM((heads, HD, rows), jnp.float32),
            pltpu.VMEM((rows, heads * HD), jnp.bfloat16),
        ],
        compiler_params=params(),
        cost_estimate=cost(2 * rows, rows, heads),
        name="close",
    )(where, ahead, *state, out_weight)


def steps(queries, keys, values, out_weight):
    chips = lax.axis_size("z")
    where = jnp.stack([lax.axis_index("z"), lax.axis_index("core"), jnp.int32(chips)]).astype(jnp.int32)
    up = [(i, (i + 1) % chips) for i in range(chips)]
    down = [(i, (i - 1) % chips) for i in range(chips)]
    swap = lambda a: lax.ppermute(a, "core", [(0, 1), (1, 0)])
    others = swap(queries)
    own = jnp.stack([keys, values])
    half = chips // 2
    ahead, behind = [own], [own]
    for k in range(1, half + 1):
        ahead.append(lax.ppermute(ahead[-1], "z", up))
        if k < half:
            behind.append(lax.ppermute(behind[-1], "z", down))
    state = open_state(where, queries, others, own)
    for k in range(1, half):
        state = fold(where, state, ahead[k], behind[k], k, k + 1 == half)
    state, (parted, stats) = state
    parted, stats = swap(parted), swap(stats)
    last = swap(ahead[half])
    mine = join(where, state, parted, stats, ahead[half], half)
    pieces = lax.axis_size("tensor")
    terms = close(where, (state[0], *mine), last, half, out_weight, pieces)
    got = lax.all_to_all(terms, "tensor", 0, 0, tiled=True)
    return jnp.sum(got.astype(jnp.float32), axis=0).astype(jnp.bfloat16)


def solution(mesh):
    finer = Mesh(
        mesh.devices.reshape(mesh.shape["parts"], mesh.shape["context"] // 2, 2, mesh.shape["tensor"]),
        ("parts", "z", "core", "tensor"),
    )
    in_specs = (
        P(PARTS_CONTEXT, "tensor"),
        P(PARTS_CONTEXT, "tensor"),
        P(PARTS_CONTEXT, "tensor"),
        P("tensor", None),
    )
    out_specs = P(PARTS_CONTEXT, "tensor")
    return jax.shard_map(steps, mesh=finer, in_specs=in_specs, out_specs=out_specs, check_vma=False)
```

```python
import jax
import jax.numpy as jnp
from jax import lax
from jax.experimental import pallas as pl
from jax.experimental.pallas import tpu as pltpu
from jax.sharding import Mesh
from jax.sharding import PartitionSpec as P

HD = 128
SIDE = 4
AWAY = (2, 1, 3)
LOWEST = -1e30
LOG2E = 1.4426950408889634
SCALE = LOG2E * HD ** (-0.5)
PARTS_CONTEXT = ("parts", "z", "core")
TENSOR = ("y", "x")
VMEM = pl.BlockSpec(memory_space=pltpu.VMEM)
SMEM = pl.BlockSpec(memory_space=pltpu.SMEM)
LIMIT = 20 * 2**20


def params():
    return pltpu.CompilerParams(vmem_limit_bytes=LIMIT)


def cost(keys, rows, heads):
    return pl.CostEstimate(
        flops=4 * keys * rows * heads * HD,
        bytes_accessed=4 * keys * HD + 4 * heads * rows * HD,
        transcendentals=keys * rows * heads,
    )


def absorb(blocks, state, first=False, diag=False):
    q_ref, top_ref, sum_ref, acc_ref = state
    heads = top_ref.shape[0]
    merge = (lambda parts: parts[0] if len(parts) == 1 else jnp.concatenate(parts, 0))
    keys = merge([b[0] for b in blocks])
    values_t = merge([b[1] for b in blocks]).T
    span = keys.shape[0]
    values_t = jnp.concatenate([values_t, jnp.ones((16, span), jnp.bfloat16)], 0)
    if diag:
        shape = (span, q_ref.shape[2])
        keep = lax.broadcasted_iota(jnp.int32, shape, 0) <= lax.broadcasted_iota(jnp.int32, shape, 1)

    def scores_of(h):
        return jnp.dot(keys, q_ref[h], preferred_element_type=jnp.float32) * SCALE

    ahead = scores_of(0)
    for h in range(heads):
        scores = ahead
        if h + 1 < heads:
            ahead = scores_of(h + 1)
        if diag:
            scores = jnp.where(keep, scores, -jnp.inf)
        top = jnp.max(scores, axis=0, keepdims=True)
        if not first:
            old = top_ref[h]
            top = jnp.maximum(old, top)
            shrink = jnp.exp2(old - top)
        weights = jnp.exp2(scores - top).astype(jnp.bfloat16)
        both = jnp.dot(values_t, weights, preferred_element_type=jnp.float32)
        acc, total = both[:HD], both[HD : HD + 1]
        top_ref[h] = top
        if first:
            sum_ref[h] = total
            acc_ref[h] = acc
        else:
            sum_ref[h] = sum_ref[h] * shrink + total
            acc_ref[h] = acc_ref[h] * shrink + acc


def sds(shape, dtype):
    return jax.ShapeDtypeStruct(shape, dtype)


def open_state(where, queries, others, own):
    rows, width = queries.shape
    heads = width // HD

    def kernel(where_ref, queries_ref, others_ref, own_ref, *state):
        for h in range(heads):
            state[0][h] = queries_ref[:, h * HD : (h + 1) * HD].T
            state[0][heads + h] = others_ref[:, h * HD : (h + 1) * HD].T
        absorb([own_ref], [r.at[:heads] for r in state], first=True, diag=True)
        rest = [r.at[heads:] for r in state]

        @pl.when(where_ref[1] == 0)
        def _():
            absorb([own_ref], rest, first=True)

        @pl.when(where_ref[1] != 0)
        def _():
            rest[1][...] = jnp.full(rest[1].shape, LOWEST, jnp.float32)
            rest[2][...] = jnp.zeros(rest[2].shape, jnp.float32)
            rest[3][...] = jnp.zeros(rest[3].shape, jnp.float32)

    return pl.pallas_call(
        kernel,
        out_shape=(
            sds((2 * heads, HD, rows), jnp.bfloat16),
            sds((2 * heads, 1, rows), jnp.float32),
            sds((2 * heads, 1, rows), jnp.float32),
            sds((2 * heads, HD, rows), jnp.float32),
        ),
        in_specs=[SMEM, VMEM, VMEM, VMEM],
        out_specs=(VMEM,) * 4,
        compiler_params=params(),
        cost_estimate=cost(rows, rows, 2 * heads),
        name="open_state",
    )(where, queries, others, own)


def fold(where, state, ahead, behind, step, parting):
    def kernel(where_ref, ahead_ref, behind_ref, *refs):
        live = refs[:4]
        z = where_ref[0]
        size = where_ref[2]

        @pl.when(z + step >= size)
        def _():
            absorb([ahead_ref, behind_ref], live)

        @pl.when((z + step < size) & (z >= step))
        def _():
            absorb([ahead_ref], live)

        if parting:
            out_ref, stat_ref = refs[-2:]
            heads = live[0].shape[0] // 2
            for h in range(heads):
                total = live[2][heads + h]
                scale = jnp.where(total > 0, 1.0 / jnp.where(total > 0, total, 1.0), 0.0)
                out_ref[h] = (live[3][heads + h] * scale).astype(jnp.bfloat16)
                stat_ref[0, h] = live[1][heads + h]
                stat_ref[1, h] = total

    heads, _, rows = state[0].shape
    extra = (sds((heads // 2, HD, rows), jnp.bfloat16), sds((2, heads // 2, 1, rows), jnp.float32)) if parting else ()
    out = pl.pallas_call(
        kernel,
        out_shape=tuple(sds(a.shape, a.dtype) for a in state) + extra,
        in_specs=[SMEM] + [VMEM] * 6,
        out_specs=(VMEM,) * (4 + len(extra)),
        input_output_aliases={3 + i: i for i in range(4)},
        compiler_params=params(),
        cost_estimate=cost(2 * ahead.shape[1], rows, heads),
    )(where, ahead, behind, *state)
    return (out[:4], out[4:]) if parting else out


def join(where, state, parted, stats, ahead, step):
    heads, _, rows = parted.shape

    def kernel(where_ref, parted_ref, stats_ref, ahead_ref, *refs):
        state_in, state_out = refs[:4], refs[4:]
        live = (state_in[0].at[:heads],) + tuple(state_out)
        for h in range(heads):
            old, theirs = state_in[1][h], stats_ref[0, h]
            top = jnp.maximum(old, theirs)
            mine = jnp.exp2(old - top)
            part = jnp.exp2(theirs - top) * stats_ref[1, h]
            state_out[0][h] = top
            state_out[1][h] = state_in[2][h] * mine + part
            state_out[2][h] = state_in[3][h] * mine + parted_ref[h].astype(jnp.float32) * part

        @pl.when(where_ref[0] >= step)
        def _():
            absorb([ahead_ref], live)

    return pl.pallas_call(
        kernel,
        out_shape=tuple(sds((heads, *a.shape[1:]), a.dtype) for a in state[1:]),
        in_specs=[SMEM] + [VMEM] * 7,
        out_specs=(VMEM,) * 3,
        compiler_params=params(),
        cost_estimate=cost(ahead.shape[1], rows, heads),
        name="join",
    )(where, parted, stats, ahead, *state)


def column(where_ref, step, flip, width):
    y = lax.rem(where_ref[3] + step, SIDE)
    x = where_ref[4] if flip == 0 else 1 - where_ref[4]
    return pl.multiple_of((y * 2 + x) * width, width)


def project(att, weight_ref, start, width):
    return jnp.dot(att, weight_ref[:, pl.ds(start, width)], preferred_element_type=jnp.float32)


def close(where, state, ahead, step, out_weight, first, width):
    heads, _, rows = state[3].shape

    def kernel(where_ref, ahead_ref, q_ref, top_ref, sum_ref, acc_ref, weight_ref, att_ref, out_ref, *scratch):
        live = (q_ref.at[:heads], *scratch)
        for src, dst in zip((top_ref, sum_ref, acc_ref), live[1:]):
            dst[...] = src[...]

        @pl.when(where_ref[0] >= step)
        def _():
            absorb([ahead_ref], live)

        for h in range(heads):
            att_ref[:, h * HD : (h + 1) * HD] = (live[3][h] / live[2][h]).T.astype(jnp.bfloat16)

        def one(d, _):
            start = column(where_ref, d, 1, width)
            out_ref[d] = project(att_ref[:first], weight_ref, start, width).astype(jnp.bfloat16)
            return 0

        lax.fori_loop(0, SIDE, one, 0)

    return pl.pallas_call(
        kernel,
        out_shape=(sds((rows, heads * HD), jnp.bfloat16), sds((SIDE, first, width), jnp.bfloat16)),
        in_specs=[SMEM] + [VMEM] * 6,
        out_specs=(VMEM,) * 2,
        scratch_shapes=[pltpu.VMEM(a.shape, a.dtype) for a in state[1:]],
        compiler_params=params(),
        cost_estimate=cost(2 * rows, rows, heads),
        name="close",
    )(where, ahead, *state, out_weight)


def project_away(where, att, out_weight, first, width):
    rows = att.shape[0] - first

    def kernel(where_ref, att_ref, weight_ref, *outs):
        for out_ref, d in zip(outs, AWAY):
            for flip in range(2):
                terms = project(att_ref[first:], weight_ref, column(where_ref, d, flip, width), width)
                out_ref[flip] = terms.astype(jnp.bfloat16)

    return pl.pallas_call(
        kernel,
        out_shape=(sds((2, rows, width), jnp.bfloat16),) * len(AWAY),
        in_specs=[SMEM, VMEM, VMEM],
        out_specs=(VMEM,) * len(AWAY),
        compiler_params=params(),
        cost_estimate=cost(2 * rows, rows, 8),
        name="project_away",
    )(where, att, out_weight)


def project_here(where, att, out_weight, first, width):
    rows = att.shape[0] - first

    def kernel(where_ref, att_ref, weight_ref, last_ref, first_ref):
        for flip in range(2):
            last_ref[flip] = project(att_ref[first:], weight_ref, column(where_ref, 0, flip, width), width)

        def one(d, _):
            first_ref[d] = project(att_ref[:first], weight_ref, column(where_ref, d, 0, width), width)
            return 0

        lax.fori_loop(0, SIDE, one, 0)

    return pl.pallas_call(
        kernel,
        out_shape=(sds((2, rows, width), jnp.float32), sds((SIDE, first, width), jnp.float32)),
        in_specs=[SMEM, VMEM, VMEM],
        out_specs=(VMEM,) * 2,
        compiler_params=params(),
        cost_estimate=cost(2 * rows, rows, 8),
        name="project_here",
    )(where, att, out_weight)


def add_first(kept, got):
    _, rows, width = kept.shape

    def kernel(kept_ref, got_ref, here_ref, *outs):
        here_ref[...] = kept_ref[0] + got_ref[0].astype(jnp.float32)
        for out_ref, d in zip(outs, AWAY):
            out_ref[...] = (kept_ref[d] + got_ref[d].astype(jnp.float32)).astype(jnp.bfloat16)

    return pl.pallas_call(
        kernel,
        out_shape=(sds((rows, width), jnp.float32),) + (sds((rows, width), jnp.bfloat16),) * len(AWAY),
        in_specs=[VMEM] * 2,
        out_specs=(VMEM,) * (1 + len(AWAY)),
        compiler_params=params(),
        cost_estimate=pl.CostEstimate(flops=kept.size, bytes_accessed=8 * kept.size, transcendentals=0),
        name="add_first",
    )(kept, got)


def add_last(kept, got):
    _, rows, width = kept.shape

    def kernel(kept_ref, *refs):
        *got_refs, here_ref, out_ref = refs
        here_ref[...] = kept_ref[0] + sum(r[0].astype(jnp.float32) for r in got_refs)
        out_ref[...] = (kept_ref[1] + sum(r[1].astype(jnp.float32) for r in got_refs)).astype(jnp.bfloat16)

    return pl.pallas_call(
        kernel,
        out_shape=(sds((rows, width), jnp.float32), sds((rows, width), jnp.bfloat16)),
        in_specs=[VMEM] * (1 + len(got)),
        out_specs=(VMEM,) * 2,
        compiler_params=params(),
        cost_estimate=pl.CostEstimate(flops=kept.size, bytes_accessed=8 * kept.size, transcendentals=0),
        name="add_last",
    )(kept, *got)


def finish(first_here, first_got, last_here, last_got):
    rows, width = first_here.shape
    more = last_here.shape[0]

    def kernel(first_ref, *refs):
        *got_refs, last_ref, swapped_ref, out_ref = refs
        out_ref[:rows] = (first_ref[...] + sum(r[...].astype(jnp.float32) for r in got_refs)).astype(jnp.bfloat16)
        out_ref[rows:] = (last_ref[...] + swapped_ref[...].astype(jnp.float32)).astype(jnp.bfloat16)

    return pl.pallas_call(
        kernel,
        out_shape=sds((rows + more, width), jnp.bfloat16),
        in_specs=[VMEM] * (3 + len(first_got)),
        out_specs=VMEM,
        compiler_params=params(),
        name="finish",
    )(first_here, *first_got, last_here, last_got)


def steps(queries, keys, values, out_weight):
    chips = lax.axis_size("z")
    where = jnp.stack([lax.axis_index("z"), lax.axis_index("core"), jnp.int32(chips), lax.axis_index("y"), lax.axis_index("x")]).astype(jnp.int32)
    up = [(i, (i + 1) % chips) for i in range(chips)]
    down = [(i, (i - 1) % chips) for i in range(chips)]
    swap = lambda a: lax.ppermute(a, "core", [(0, 1), (1, 0)])
    others = swap(queries)
    own = jnp.stack([keys, values])
    half = chips // 2
    ahead, behind = [own], [own]
    for k in range(1, half + 1):
        ahead.append(lax.ppermute(ahead[-1], "z", up))
        if k < half:
            behind.append(lax.ppermute(behind[-1], "z", down))
    state = open_state(where, queries, others, own)
    for k in range(1, half):
        state = fold(where, state, ahead[k], behind[k], k, k + 1 == half)
    state, (parted, stats) = state
    parted, stats = swap(parted), swap(stats)
    last = swap(ahead[half])
    mine = join(where, state, parted, stats, ahead[half], half)
    width = out_weight.shape[1] // (2 * SIDE)
    first = queries.shape[0] // 2
    att, send = close(where, (state[0], *mine), last, half, out_weight, first, width)
    across = lambda a: lax.ppermute(a, "x", [(0, 1), (1, 0)])
    along = lambda a, d: lax.ppermute(a, "y", [(i, (i + d) % SIDE) for i in range(SIDE)])
    got_x = across(send)
    away = project_away(where, att, out_weight, first, width)
    got_y = [along(a, d) for a, d in zip(away, AWAY)]
    last_kept, first_kept = project_here(where, att, out_weight, first, width)
    first_here, *first_away = add_first(first_kept, got_x)
    first_got = [along(a, d) for a, d in zip(first_away, AWAY)]
    last_here, last_away = add_last(last_kept, got_y)
    last_got = across(last_away)
    return finish(first_here, first_got, last_here, last_got)


def solution(mesh):
    finer = Mesh(
        mesh.devices.reshape(mesh.shape["parts"], mesh.shape["context"] // 2, 2, SIDE, mesh.shape["tensor"] // SIDE),
        ("parts", "z", "core", "y", "x"),
    )
    in_specs = (
        P(PARTS_CONTEXT, TENSOR),
        P(PARTS_CONTEXT, TENSOR),
        P(PARTS_CONTEXT, TENSOR),
        P(TENSOR, None),
    )
    out_specs = P(PARTS_CONTEXT, TENSOR)
    return jax.shard_map(steps, mesh=finer, in_specs=in_specs, out_specs=out_specs, check_vma=False)
```

```python
import jax
import jax.numpy as jnp
from jax import lax
from jax.experimental import pallas as pl
from jax.experimental.pallas import tpu as pltpu
from jax.sharding import Mesh
from jax.sharding import PartitionSpec as P

HD = 128
SIDE = 4
AWAY = (1, 3, 2)
LOWEST = -1e30
LOG2E = 1.4426950408889634
SCALE = LOG2E * HD ** (-0.5)
PARTS_CONTEXT = ("parts", "z", "core")
TENSOR = ("y", "x")
VMEM = pl.BlockSpec(memory_space=pltpu.VMEM)
SMEM = pl.BlockSpec(memory_space=pltpu.SMEM)
LIMIT = 20 * 2**20


def params():
    return pltpu.CompilerParams(vmem_limit_bytes=LIMIT)


def cost(keys, rows, heads):
    return pl.CostEstimate(
        flops=4 * keys * rows * heads * HD,
        bytes_accessed=4 * keys * HD + 4 * heads * rows * HD,
        transcendentals=keys * rows * heads,
    )


def absorb(blocks, state, first=False, diag=False):
    q_ref, top_ref, sum_ref, acc_ref = state
    heads = top_ref.shape[0]
    merge = (lambda parts: parts[0] if len(parts) == 1 else jnp.concatenate(parts, 0))
    keys = merge([b[0] for b in blocks])
    values_t = merge([b[1] for b in blocks]).T
    span = keys.shape[0]
    values_t = jnp.concatenate([values_t, jnp.ones((16, span), jnp.bfloat16)], 0)
    if diag:
        shape = (span, q_ref.shape[2])
        keep = lax.broadcasted_iota(jnp.int32, shape, 0) <= lax.broadcasted_iota(jnp.int32, shape, 1)

    def scores_of(h):
        return jnp.dot(keys, q_ref[h], preferred_element_type=jnp.float32) * SCALE

    def settle(h, weights, top, shrink):
        both = jnp.dot(values_t, weights, preferred_element_type=jnp.float32)
        acc, total = both[:HD], both[HD : HD + 1]
        top_ref[h] = top
        if first:
            sum_ref[h] = total
            acc_ref[h] = acc
        else:
            sum_ref[h] = sum_ref[h] * shrink + total
            acc_ref[h] = acc_ref[h] * shrink + acc

    ahead = [scores_of(h) for h in range(2)]
    waiting = None
    for h in range(heads):
        scores = ahead.pop(0)
        if h + 2 < heads:
            ahead.append(scores_of(h + 2))
        if diag:
            scores = jnp.where(keep, scores, -jnp.inf)
        top = jnp.max(scores, axis=0, keepdims=True)
        shrink = None
        if not first:
            old = top_ref[h]
            top = jnp.maximum(old, top)
            shrink = jnp.exp2(old - top)
        weights = jnp.exp2(scores - top).astype(jnp.bfloat16)
        if waiting:
            settle(*waiting)
        waiting = (h, weights, top, shrink)
    settle(*waiting)


def sds(shape, dtype):
    return jax.ShapeDtypeStruct(shape, dtype)


def turned(queries_ref, out_ref):
    for h in range(out_ref.shape[0]):
        out_ref[h] = queries_ref[:, h * HD : (h + 1) * HD].T


def open_state(where, queries, others, own):
    rows, width = queries.shape
    heads = width // HD

    def kernel(where_ref, queries_ref, others_ref, own_ref, *state):
        live = [r.at[:heads] for r in state]
        rest = [r.at[heads:] for r in state]
        turned(queries_ref, live[0])
        turned(others_ref, rest[0])
        absorb([own_ref], live, first=True, diag=True)

        @pl.when(where_ref[1] == 0)
        def _():
            absorb([own_ref], rest, first=True)

        @pl.when(where_ref[1] != 0)
        def _():
            rest[1][...] = jnp.full(rest[1].shape, LOWEST, jnp.float32)
            rest[2][...] = jnp.zeros(rest[2].shape, jnp.float32)
            rest[3][...] = jnp.zeros(rest[3].shape, jnp.float32)

    return pl.pallas_call(
        kernel,
        out_shape=(
            sds((2 * heads, HD, rows), jnp.bfloat16),
            sds((2 * heads, 1, rows), jnp.float32),
            sds((2 * heads, 1, rows), jnp.float32),
            sds((2 * heads, HD, rows), jnp.float32),
        ),
        in_specs=[SMEM, VMEM, VMEM, VMEM],
        out_specs=(VMEM,) * 4,
        compiler_params=params(),
        cost_estimate=cost(rows, rows, 2 * heads),
        name="open_state",
    )(where, queries, others, own)


def fold(where, state, ahead, behind, step, parting=False, heads=None):
    def kernel(where_ref, ahead_ref, behind_ref, *refs):
        live = refs[:4] if heads is None else [r.at[:heads] for r in refs[:4]]
        z = where_ref[0]
        size = where_ref[2]

        @pl.when(z + step >= size)
        def _():
            absorb([ahead_ref, behind_ref], live)

        @pl.when((z + step < size) & (z >= step))
        def _():
            def part(i, _):
                absorb([ahead_ref], [r.at[pl.ds(i * 4, 4)] for r in live])
                return 0

            lax.fori_loop(0, live[1].shape[0] // 4, part, 0)

        if parting:
            out_ref, stat_ref = refs[-2:]
            half = live[0].shape[0] // 2
            for h in range(half):
                total = live[2][half + h]
                scale = jnp.where(total > 0, 1.0 / jnp.where(total > 0, total, 1.0), 0.0)
                out_ref[h] = (live[3][half + h] * scale).astype(jnp.bfloat16)
                stat_ref[0, h] = live[1][half + h]
                stat_ref[1, h] = total

    full, _, rows = state[0].shape
    extra = (sds((full // 2, HD, rows), jnp.bfloat16), sds((2, full // 2, 1, rows), jnp.float32)) if parting else ()
    out = pl.pallas_call(
        kernel,
        out_shape=tuple(sds(a.shape, a.dtype) for a in state) + extra,
        in_specs=[SMEM] + [VMEM] * 6,
        out_specs=(VMEM,) * (4 + len(extra)),
        input_output_aliases={3 + i: i for i in range(4)},
        compiler_params=params(),
        cost_estimate=cost(2 * ahead.shape[1], rows, heads or full),
    )(where, ahead, behind, *state)
    return (out[:4], out[4:]) if parting else out


def join(where, state, parted, stats, ahead, step):
    heads, _, rows = parted.shape

    def kernel(where_ref, parted_ref, stats_ref, ahead_ref, *refs):
        state_in, state_out = refs[:4], refs[4:]
        live = (state_in[0].at[:heads],) + tuple(state_out)
        for h in range(heads):
            old, theirs = state_in[1][h], stats_ref[0, h]
            top = jnp.maximum(old, theirs)
            mine = jnp.exp2(old - top)
            part = jnp.exp2(theirs - top) * stats_ref[1, h]
            state_out[0][h] = top
            state_out[1][h] = state_in[2][h] * mine + part
            state_out[2][h] = state_in[3][h] * mine + parted_ref[h].astype(jnp.float32) * part

        @pl.when(where_ref[0] >= step)
        def _():
            absorb([ahead_ref], live)

    return pl.pallas_call(
        kernel,
        out_shape=tuple(sds((heads, *a.shape[1:]), a.dtype) for a in state[1:]),
        in_specs=[SMEM] + [VMEM] * 7,
        out_specs=(VMEM,) * 3,
        compiler_params=params(),
        cost_estimate=cost(ahead.shape[1], rows, heads),
        name="join",
    )(where, parted, stats, ahead, *state)


def column(where_ref, step, flip, width):
    y = lax.rem(where_ref[3] + step, SIDE)
    x = where_ref[4] if flip == 0 else 1 - where_ref[4]
    return pl.multiple_of((y * 2 + x) * width, width)


def project(att, weight_ref, start, width):
    return jnp.dot(att, weight_ref[:, pl.ds(start, width)], preferred_element_type=jnp.float32)


def close(where, state, ahead, step, out_weight, first, width):
    heads, _, rows = state[3].shape

    def kernel(where_ref, ahead_ref, q_ref, top_ref, sum_ref, acc_ref, weight_ref, att_ref, out_ref, *scratch):
        live = (q_ref.at[:heads], *scratch)
        for src, dst in zip((top_ref, sum_ref, acc_ref), live[1:]):
            dst[...] = src[...]

        @pl.when(where_ref[0] >= step)
        def _():
            absorb([ahead_ref], live)

        for h in range(heads):
            att_ref[:, h * HD : (h + 1) * HD] = (live[3][h] * (1.0 / live[2][h])).astype(jnp.bfloat16).T

        def one(d, _):
            start = column(where_ref, d, 1, width)
            out_ref[d] = project(att_ref[:first], weight_ref, start, width).astype(jnp.bfloat16)
            return 0

        lax.fori_loop(0, SIDE, one, 0)

    return pl.pallas_call(
        kernel,
        out_shape=(sds((rows, heads * HD), jnp.bfloat16), sds((SIDE, first, width), jnp.bfloat16)),
        in_specs=[SMEM] + [VMEM] * 6,
        out_specs=(VMEM,) * 2,
        scratch_shapes=[pltpu.VMEM(a.shape, a.dtype) for a in state[1:]],
        compiler_params=params(),
        cost_estimate=cost(2 * rows, rows, heads),
        name="close",
    )(where, ahead, *state, out_weight)


def project_away(where, att, out_weight, first, width):
    rows = att.shape[0] - first

    def kernel(where_ref, att_ref, weight_ref, *outs):
        for out_ref, d in zip(outs, AWAY):
            for flip in range(2):
                terms = project(att_ref[first:], weight_ref, column(where_ref, d, flip, width), width)
                out_ref[flip] = terms.astype(jnp.bfloat16)

    return pl.pallas_call(
        kernel,
        out_shape=(sds((2, rows, width), jnp.bfloat16),) * len(AWAY),
        in_specs=[SMEM, VMEM, VMEM],
        out_specs=(VMEM,) * len(AWAY),
        compiler_params=params(),
        cost_estimate=cost(2 * rows, rows, 8),
        name="project_away",
    )(where, att, out_weight)


def project_here(where, att, out_weight, first, width):
    rows = att.shape[0] - first

    def kernel(where_ref, att_ref, weight_ref, last_ref, first_ref):
        for flip in range(2):
            last_ref[flip] = project(att_ref[first:], weight_ref, column(where_ref, 0, flip, width), width)

        def one(d, _):
            first_ref[d] = project(att_ref[:first], weight_ref, column(where_ref, d, 0, width), width)
            return 0

        lax.fori_loop(0, SIDE, one, 0)

    return pl.pallas_call(
        kernel,
        out_shape=(sds((2, rows, width), jnp.float32), sds((SIDE, first, width), jnp.float32)),
        in_specs=[SMEM, VMEM, VMEM],
        out_specs=(VMEM,) * 2,
        compiler_params=params(),
        cost_estimate=cost(2 * rows, rows, 8),
        name="project_here",
    )(where, att, out_weight)


def add_first(kept, got):
    _, rows, width = kept.shape

    def kernel(kept_ref, got_ref, here_ref, *outs):
        here_ref[...] = kept_ref[0] + got_ref[0].astype(jnp.float32)
        for out_ref, d in zip(outs, AWAY):
            out_ref[...] = (kept_ref[d] + got_ref[d].astype(jnp.float32)).astype(jnp.bfloat16)

    return pl.pallas_call(
        kernel,
        out_shape=(sds((rows, width), jnp.float32),) + (sds((rows, width), jnp.bfloat16),) * len(AWAY),
        in_specs=[VMEM] * 2,
        out_specs=(VMEM,) * (1 + len(AWAY)),
        compiler_params=params(),
        cost_estimate=pl.CostEstimate(flops=kept.size, bytes_accessed=8 * kept.size, transcendentals=0),
        name="add_first",
    )(kept, got)


def add_last(kept, got):
    _, rows, width = kept.shape

    def kernel(kept_ref, *refs):
        *got_refs, here_ref, out_ref = refs
        here_ref[...] = kept_ref[0] + sum(r[0].astype(jnp.float32) for r in got_refs)
        out_ref[...] = (kept_ref[1] + sum(r[1].astype(jnp.float32) for r in got_refs)).astype(jnp.bfloat16)

    return pl.pallas_call(
        kernel,
        out_shape=(sds((rows, width), jnp.float32), sds((rows, width), jnp.bfloat16)),
        in_specs=[VMEM] * (1 + len(got)),
        out_specs=(VMEM,) * 2,
        compiler_params=params(),
        cost_estimate=pl.CostEstimate(flops=kept.size, bytes_accessed=8 * kept.size, transcendentals=0),
        name="add_last",
    )(kept, *got)


def finish(first_here, first_got, last_here, last_got):
    rows, width = first_here.shape
    more = last_here.shape[0]

    def kernel(first_ref, *refs):
        *got_refs, last_ref, swapped_ref, out_ref = refs
        out_ref[:rows] = (first_ref[...] + sum(r[...].astype(jnp.float32) for r in got_refs)).astype(jnp.bfloat16)
        out_ref[rows:] = (last_ref[...] + swapped_ref[...].astype(jnp.float32)).astype(jnp.bfloat16)

    return pl.pallas_call(
        kernel,
        out_shape=sds((rows + more, width), jnp.bfloat16),
        in_specs=[VMEM] * (3 + len(first_got)),
        out_specs=VMEM,
        compiler_params=params(),
        name="finish",
    )(first_here, *first_got, last_here, last_got)


def steps(queries, keys, values, out_weight):
    chips = lax.axis_size("z")
    where = jnp.stack([lax.axis_index("z"), lax.axis_index("core"), jnp.int32(chips), lax.axis_index("y"), lax.axis_index("x")]).astype(jnp.int32)
    up = [(i, (i + 1) % chips) for i in range(chips)]
    down = [(i, (i - 1) % chips) for i in range(chips)]
    swap = lambda a: lax.ppermute(a, "core", [(0, 1), (1, 0)])
    own = jnp.stack([keys, values])
    others = swap(queries)
    half = chips // 2
    heads = queries.shape[1] // HD
    ahead, behind = [own], [own]
    for k in range(1, half + 1):
        ahead.append(lax.ppermute(ahead[-1], "z", up))
        if k < half:
            behind.append(lax.ppermute(behind[-1], "z", down))
    state = open_state(where, queries, others, own)
    for k in range(1, half - 1):
        state = fold(where, state, ahead[k], behind[k], k, k + 2 == half)
    state, (parted, stats) = state
    k = half - 1
    swap_ahead, swap_behind = swap(ahead[k]), swap(behind[k])
    parted, stats = swap(parted), swap(stats)
    state = fold(where, state, ahead[k], behind[k], k, heads=heads)
    state = fold(where, state, swap_ahead, swap_behind, k, heads=heads)
    last = swap(ahead[half])
    mine = join(where, state, parted, stats, ahead[half], half)
    width = out_weight.shape[1] // (2 * SIDE)
    first = queries.shape[0] // 2
    att, send = close(where, (state[0], *mine), last, half, out_weight, first, width)
    across = lambda a: lax.ppermute(a, "x", [(0, 1), (1, 0)])
    along = lambda a, d: lax.ppermute(a, "y", [(i, (i + d) % SIDE) for i in range(SIDE)])
    got_x = across(send)
    away = project_away(where, att, out_weight, first, width)
    got_y = [along(a, d) for a, d in zip(away, AWAY)]
    last_kept, first_kept = project_here(where, att, out_weight, first, width)
    first_here, *first_away = add_first(first_kept, got_x)
    first_got = [along(a, d) for a, d in zip(first_away, AWAY)]
    last_here, last_away = add_last(last_kept, got_y)
    last_got = across(last_away)
    return finish(first_here, first_got, last_here, last_got)


def solution(mesh):
    finer = Mesh(
        mesh.devices.reshape(mesh.shape["parts"], mesh.shape["context"] // 2, 2, SIDE, mesh.shape["tensor"] // SIDE),
        ("parts", "z", "core", "y", "x"),
    )
    in_specs = (
        P(PARTS_CONTEXT, TENSOR),
        P(PARTS_CONTEXT, TENSOR),
        P(PARTS_CONTEXT, TENSOR),
        P(TENSOR, None),
    )
    out_specs = P(PARTS_CONTEXT, TENSOR)
    return jax.shard_map(steps, mesh=finer, in_specs=in_specs, out_specs=out_specs, check_vma=False)
```

```python
import jax
import jax.numpy as jnp
from jax import lax
from jax.experimental import pallas as pl
from jax.experimental.pallas import tpu as pltpu
from jax.sharding import Mesh
from jax.sharding import PartitionSpec as P

HD = 128
SIDE = 4
FAR = 2
AWAY = (1, 3)
NEAR = (0, 1, 3)
LOWEST = -1e30
LOG2E = 1.4426950408889634
SCALE = LOG2E * HD ** (-0.5)
PARTS_CONTEXT = ("parts", "z", "core")
TENSOR = ("y", "x")
VMEM = pl.BlockSpec(memory_space=pltpu.VMEM)
SMEM = pl.BlockSpec(memory_space=pltpu.SMEM)
LIMIT = 20 * 2**20


def params():
    return pltpu.CompilerParams(vmem_limit_bytes=LIMIT)


def cost(keys, rows, heads):
    return pl.CostEstimate(
        flops=4 * keys * rows * heads * HD,
        bytes_accessed=4 * keys * HD + 4 * heads * rows * HD,
        transcendentals=keys * rows * heads,
    )


def absorb(blocks, state, first=False, diag=False):
    q_ref, top_ref, sum_ref, acc_ref = state
    heads = top_ref.shape[0]
    merge = (lambda parts: parts[0] if len(parts) == 1 else jnp.concatenate(parts, 0))
    keys = merge([b[0] for b in blocks])
    values_t = merge([b[1] for b in blocks]).T
    span = keys.shape[0]
    values_t = jnp.concatenate([values_t, jnp.ones((16, span), jnp.bfloat16)], 0)
    if diag:
        shape = (span, q_ref.shape[2])
        keep = lax.broadcasted_iota(jnp.int32, shape, 0) <= lax.broadcasted_iota(jnp.int32, shape, 1)

    def scores_of(h):
        return jnp.dot(keys, q_ref[h], preferred_element_type=jnp.float32) * SCALE

    def settle(h, weights, top, shrink):
        both = jnp.dot(values_t, weights, preferred_element_type=jnp.float32)
        acc, total = both[:HD], both[HD : HD + 1]
        top_ref[h] = top
        if first:
            sum_ref[h] = total
            acc_ref[h] = acc
        else:
            sum_ref[h] = sum_ref[h] * shrink + total
            acc_ref[h] = acc_ref[h] * shrink + acc

    ahead = [scores_of(h) for h in range(2)]
    waiting = None
    for h in range(heads):
        scores = ahead.pop(0)
        if h + 2 < heads:
            ahead.append(scores_of(h + 2))
        if diag:
            scores = jnp.where(keep, scores, -jnp.inf)
        top = jnp.max(scores, axis=0, keepdims=True)
        shrink = None
        if not first:
            old = top_ref[h]
            top = jnp.maximum(old, top)
            shrink = jnp.exp2(old - top)
        weights = jnp.exp2(scores - top).astype(jnp.bfloat16)
        if waiting:
            settle(*waiting)
        waiting = (h, weights, top, shrink)
    settle(*waiting)


def sds(shape, dtype):
    return jax.ShapeDtypeStruct(shape, dtype)


def turned(queries_ref, out_ref):
    for h in range(out_ref.shape[0]):
        out_ref[h] = queries_ref[:, h * HD : (h + 1) * HD].T


def open_state(where, queries, others, own):
    rows, width = queries.shape
    heads = width // HD

    def kernel(where_ref, queries_ref, others_ref, own_ref, *state):
        live = [r.at[:heads] for r in state]
        rest = [r.at[heads:] for r in state]
        turned(queries_ref, live[0])
        turned(others_ref, rest[0])
        absorb([own_ref], live, first=True, diag=True)

        @pl.when(where_ref[1] == 0)
        def _():
            absorb([own_ref], rest, first=True)

        @pl.when(where_ref[1] != 0)
        def _():
            rest[1][...] = jnp.full(rest[1].shape, LOWEST, jnp.float32)
            rest[2][...] = jnp.zeros(rest[2].shape, jnp.float32)
            rest[3][...] = jnp.zeros(rest[3].shape, jnp.float32)

    return pl.pallas_call(
        kernel,
        out_shape=(
            sds((2 * heads, HD, rows), jnp.bfloat16),
            sds((2 * heads, 1, rows), jnp.float32),
            sds((2 * heads, 1, rows), jnp.float32),
            sds((2 * heads, HD, rows), jnp.float32),
        ),
        in_specs=[SMEM, VMEM, VMEM, VMEM],
        out_specs=(VMEM,) * 4,
        compiler_params=params(),
        cost_estimate=cost(rows, rows, 2 * heads),
        name="open_state",
    )(where, queries, others, own)


def fold(where, state, ahead, behind, step, parting=False, heads=None):
    def kernel(where_ref, ahead_ref, behind_ref, *refs):
        live = refs[:4] if heads is None else [r.at[:heads] for r in refs[:4]]
        z = where_ref[0]
        size = where_ref[2]

        @pl.when(z + step >= size)
        def _():
            absorb([ahead_ref, behind_ref], live)

        @pl.when((z + step < size) & (z >= step))
        def _():
            def part(i, _):
                absorb([ahead_ref], [r.at[pl.ds(i * 4, 4)] for r in live])
                return 0

            lax.fori_loop(0, live[1].shape[0] // 4, part, 0)

        if parting:
            out_ref, stat_ref = refs[-2:]
            half = live[0].shape[0] // 2
            for h in range(half):
                total = live[2][half + h]
                scale = jnp.where(total > 0, 1.0 / jnp.where(total > 0, total, 1.0), 0.0)
                out_ref[h] = (live[3][half + h] * scale).astype(jnp.bfloat16)
                stat_ref[0, h] = live[1][half + h]
                stat_ref[1, h] = total

    full, _, rows = state[0].shape
    extra = (sds((full // 2, HD, rows), jnp.bfloat16), sds((2, full // 2, 1, rows), jnp.float32)) if parting else ()
    out = pl.pallas_call(
        kernel,
        out_shape=tuple(sds(a.shape, a.dtype) for a in state) + extra,
        in_specs=[SMEM] + [VMEM] * 6,
        out_specs=(VMEM,) * (4 + len(extra)),
        input_output_aliases={3 + i: i for i in range(4)},
        compiler_params=params(),
        cost_estimate=cost(2 * ahead.shape[1], rows, heads or full),
    )(where, ahead, behind, *state)
    return (out[:4], out[4:]) if parting else out


def join(where, state, parted, stats, ahead, step):
    heads, _, rows = parted.shape

    def kernel(where_ref, parted_ref, stats_ref, ahead_ref, *refs):
        state_in, state_out = refs[:4], refs[4:]
        live = (state_in[0].at[:heads],) + tuple(state_out)
        for h in range(heads):
            old, theirs = state_in[1][h], stats_ref[0, h]
            top = jnp.maximum(old, theirs)
            mine = jnp.exp2(old - top)
            part = jnp.exp2(theirs - top) * stats_ref[1, h]
            state_out[0][h] = top
            state_out[1][h] = state_in[2][h] * mine + part
            state_out[2][h] = state_in[3][h] * mine + parted_ref[h].astype(jnp.float32) * part

        @pl.when(where_ref[0] >= step)
        def _():
            absorb([ahead_ref], live)

    return pl.pallas_call(
        kernel,
        out_shape=tuple(sds((heads, *a.shape[1:]), a.dtype) for a in state[1:]),
        in_specs=[SMEM] + [VMEM] * 7,
        out_specs=(VMEM,) * 3,
        compiler_params=params(),
        cost_estimate=cost(ahead.shape[1], rows, heads),
        name="join",
    )(where, parted, stats, ahead, *state)


def column(where_ref, step, flip, width):
    y = lax.rem(where_ref[3] + step, SIDE)
    x = where_ref[4] if flip == 0 else 1 - where_ref[4]
    return pl.multiple_of((y * 2 + x) * width, width)


def project(att, weight_ref, start, width):
    return jnp.dot(att, weight_ref[:, pl.ds(start, width)], preferred_element_type=jnp.float32)


def close(where, state, ahead, step, out_weight, first, width):
    heads, _, rows = state[3].shape

    def kernel(where_ref, ahead_ref, q_ref, top_ref, sum_ref, acc_ref, weight_ref, att_ref, out_ref, *scratch):
        live = (q_ref.at[:heads], *scratch)
        for src, dst in zip((top_ref, sum_ref, acc_ref), live[1:]):
            dst[...] = src[...]

        @pl.when(where_ref[0] >= step)
        def _():
            absorb([ahead_ref], live)

        for h in range(heads):
            att_ref[:, h * HD : (h + 1) * HD] = (live[3][h] * (1.0 / live[2][h])).astype(jnp.bfloat16).T

        out_ref[:rows] = project(att_ref[...], weight_ref, column(where_ref, FAR, 1, width), width).astype(jnp.bfloat16)
        for i, d in enumerate(NEAR):
            terms = project(att_ref[:first], weight_ref, column(where_ref, d, 1, width), width)
            out_ref[rows + i * first : rows + (i + 1) * first] = terms.astype(jnp.bfloat16)

    return pl.pallas_call(
        kernel,
        out_shape=(sds((rows, heads * HD), jnp.bfloat16), sds((rows + len(NEAR) * first, width), jnp.bfloat16)),
        in_specs=[SMEM] + [VMEM] * 6,
        out_specs=(VMEM,) * 2,
        scratch_shapes=[pltpu.VMEM(a.shape, a.dtype) for a in state[1:]],
        compiler_params=params(),
        cost_estimate=cost(2 * rows, rows, heads),
        name="close",
    )(where, ahead, *state, out_weight)


def project_away(where, att, out_weight, first, width):
    rows = att.shape[0] - first

    def kernel(where_ref, att_ref, weight_ref, *outs):
        for out_ref, d in zip(outs, AWAY):
            for flip in range(2):
                terms = project(att_ref[first:], weight_ref, column(where_ref, d, flip, width), width)
                out_ref[flip] = terms.astype(jnp.bfloat16)

    return pl.pallas_call(
        kernel,
        out_shape=(sds((2, rows, width), jnp.bfloat16),) * len(AWAY),
        in_specs=[SMEM, VMEM, VMEM],
        out_specs=(VMEM,) * len(AWAY),
        compiler_params=params(),
        cost_estimate=cost(2 * rows, rows, 8),
        name="project_away",
    )(where, att, out_weight)


def project_here(where, att, out_weight, first, width):
    full = att.shape[0]
    rows = full - first

    def kernel(where_ref, att_ref, weight_ref, last_ref, first_ref):
        for flip in range(2):
            last_ref[flip] = project(att_ref[first:], weight_ref, column(where_ref, 0, flip, width), width)
        first_ref[:full] = project(att_ref[...], weight_ref, column(where_ref, FAR, 0, width), width)
        for i, d in enumerate(NEAR):
            terms = project(att_ref[:first], weight_ref, column(where_ref, d, 0, width), width)
            first_ref[full + i * first : full + (i + 1) * first] = terms

    return pl.pallas_call(
        kernel,
        out_shape=(sds((2, rows, width), jnp.float32), sds((full + len(NEAR) * first, width), jnp.float32)),
        in_specs=[SMEM, VMEM, VMEM],
        out_specs=(VMEM,) * 2,
        compiler_params=params(),
        cost_estimate=cost(2 * rows, rows, 8),
        name="project_here",
    )(where, att, out_weight)


def add_first(kept, got, first):
    total, width = kept.shape
    full = total - len(NEAR) * first

    def kernel(kept_ref, got_ref, here_ref, far_ref, *outs):
        far_ref[...] = (kept_ref[:full] + got_ref[:full].astype(jnp.float32)).astype(jnp.bfloat16)
        for i, out_ref in enumerate((here_ref, *outs)):
            here = slice(full + i * first, full + (i + 1) * first)
            out_ref[...] = (kept_ref[here] + got_ref[here].astype(jnp.float32)).astype(out_ref.dtype)

    near = sds((first, width), jnp.bfloat16)
    return pl.pallas_call(
        kernel,
        out_shape=(sds((first, width), jnp.float32), sds((full, width), jnp.bfloat16)) + (near,) * len(AWAY),
        in_specs=[VMEM] * 2,
        out_specs=(VMEM,) * (2 + len(AWAY)),
        compiler_params=params(),
        cost_estimate=pl.CostEstimate(flops=kept.size, bytes_accessed=8 * kept.size, transcendentals=0),
        name="add_first",
    )(kept, got)


def add_last(kept, got):
    _, rows, width = kept.shape

    def kernel(kept_ref, *refs):
        *got_refs, here_ref, out_ref = refs
        here_ref[...] = kept_ref[0] + sum(r[0].astype(jnp.float32) for r in got_refs)
        out_ref[...] = (kept_ref[1] + sum(r[1].astype(jnp.float32) for r in got_refs)).astype(jnp.bfloat16)

    return pl.pallas_call(
        kernel,
        out_shape=(sds((rows, width), jnp.float32), sds((rows, width), jnp.bfloat16)),
        in_specs=[VMEM] * (1 + len(got)),
        out_specs=(VMEM,) * 2,
        compiler_params=params(),
        cost_estimate=pl.CostEstimate(flops=kept.size, bytes_accessed=8 * kept.size, transcendentals=0),
        name="add_last",
    )(kept, *got)


def finish(first_here, first_got, far_got, last_here, last_got):
    rows, width = first_here.shape
    more = last_here.shape[0]

    def kernel(first_ref, *refs):
        *got_refs, far_ref, last_ref, swapped_ref, out_ref = refs
        far = far_ref[...].astype(jnp.float32)
        out_ref[:rows] = (first_ref[...] + far[:rows] + sum(r[...].astype(jnp.float32) for r in got_refs)).astype(jnp.bfloat16)
        out_ref[rows:] = (last_ref[...] + far[rows:] + swapped_ref[...].astype(jnp.float32)).astype(jnp.bfloat16)

    return pl.pallas_call(
        kernel,
        out_shape=sds((rows + more, width), jnp.bfloat16),
        in_specs=[VMEM] * (4 + len(first_got)),
        out_specs=VMEM,
        compiler_params=params(),
        name="finish",
    )(first_here, *first_got, far_got, last_here, last_got)


def steps(queries, keys, values, out_weight):
    chips = lax.axis_size("z")
    where = jnp.stack([lax.axis_index("z"), lax.axis_index("core"), jnp.int32(chips), lax.axis_index("y"), lax.axis_index("x")]).astype(jnp.int32)
    up = [(i, (i + 1) % chips) for i in range(chips)]
    down = [(i, (i - 1) % chips) for i in range(chips)]
    swap = lambda a: lax.ppermute(a, "core", [(0, 1), (1, 0)])
    own = jnp.stack([keys, values])
    others = swap(queries)
    half = chips // 2
    heads = queries.shape[1] // HD
    ahead, behind = [own], [own]
    for k in range(1, half + 1):
        ahead.append(lax.ppermute(ahead[-1], "z", up))
        if k < half:
            behind.append(lax.ppermute(behind[-1], "z", down))
    state = open_state(where, queries, others, own)
    for k in range(1, half - 1):
        state = fold(where, state, ahead[k], behind[k], k, k + 2 == half)
    state, (parted, stats) = state
    k = half - 1
    swap_ahead, swap_behind = swap(ahead[k]), swap(behind[k])
    parted, stats = swap(parted), swap(stats)
    state = fold(where, state, ahead[k], behind[k], k, heads=heads)
    state = fold(where, state, swap_ahead, swap_behind, k, heads=heads)
    last = swap(ahead[half])
    mine = join(where, state, parted, stats, ahead[half], half)
    width = out_weight.shape[1] // (2 * SIDE)
    first = queries.shape[0] * 4 // 16
    att, send = close(where, (state[0], *mine), last, half, out_weight, first, width)
    across = lambda a: lax.ppermute(a, "x", [(0, 1), (1, 0)])
    along = lambda a, d: lax.ppermute(a, "y", [(i, (i + d) % SIDE) for i in range(SIDE)])
    got_x = across(send)
    away = project_away(where, att, out_weight, first, width)
    got_y = [along(a, d) for a, d in zip(away, AWAY)]
    last_kept, first_kept = project_here(where, att, out_weight, first, width)
    first_here, far_away, *first_away = add_first(first_kept, got_x, first)
    far_got = along(far_away, FAR)
    first_got = [along(a, d) for a, d in zip(first_away, AWAY)]
    last_here, last_away = add_last(last_kept, got_y)
    last_got = across(last_away)
    return finish(first_here, first_got, far_got, last_here, last_got)


def solution(mesh):
    finer = Mesh(
        mesh.devices.reshape(mesh.shape["parts"], mesh.shape["context"] // 2, 2, SIDE, mesh.shape["tensor"] // SIDE),
        ("parts", "z", "core", "y", "x"),
    )
    in_specs = (
        P(PARTS_CONTEXT, TENSOR),
        P(PARTS_CONTEXT, TENSOR),
        P(PARTS_CONTEXT, TENSOR),
        P(TENSOR, None),
    )
    out_specs = P(PARTS_CONTEXT, TENSOR)
    return jax.shard_map(steps, mesh=finer, in_specs=in_specs, out_specs=out_specs, check_vma=False)
```

```python
import jax
import jax.numpy as jnp
from jax import lax
from jax.experimental import pallas as pl
from jax.experimental.pallas import tpu as pltpu
from jax.sharding import Mesh
from jax.sharding import PartitionSpec as P

HD = 128
SIDE = 4
FAR = 2
AWAY = (1, 3)
NEAR = (0, 1, 3)
LOWEST = -1e30
LOG2E = 1.4426950408889634
SCALE = LOG2E * HD ** (-0.5)
PARTS_CONTEXT = ("parts", "z", "core")
TENSOR = ("y", "x")
VMEM = pl.BlockSpec(memory_space=pltpu.VMEM)
SMEM = pl.BlockSpec(memory_space=pltpu.SMEM)
LIMIT = 20 * 2**20


def params():
    return pltpu.CompilerParams(vmem_limit_bytes=LIMIT)


def cost(keys, rows, heads):
    return pl.CostEstimate(
        flops=4 * keys * rows * heads * HD,
        bytes_accessed=4 * keys * HD + 4 * heads * rows * HD,
        transcendentals=keys * rows * heads,
    )


def absorb(blocks, state, first=False, diag=False):
    q_ref, top_ref, sum_ref, acc_ref = state
    heads = top_ref.shape[0]
    merge = (lambda parts: parts[0] if len(parts) == 1 else jnp.concatenate(parts, 0))
    keys = merge([b[0] for b in blocks])
    values_t = merge([b[1] for b in blocks]).T
    span = keys.shape[0]
    values_t = jnp.concatenate([values_t, jnp.ones((16, span), jnp.bfloat16)], 0)
    if diag:
        shape = (span, q_ref.shape[2])
        keep = lax.broadcasted_iota(jnp.int32, shape, 0) <= lax.broadcasted_iota(jnp.int32, shape, 1)

    def scores_of(h):
        return jnp.dot(keys, q_ref[h], preferred_element_type=jnp.float32) * SCALE

    def settle(h, weights, top, shrink):
        both = jnp.dot(values_t, weights, preferred_element_type=jnp.float32)
        acc, total = both[:HD], both[HD : HD + 1]
        top_ref[h] = top
        if first:
            sum_ref[h] = total
            acc_ref[h] = acc
        else:
            sum_ref[h] = sum_ref[h] * shrink + total
            acc_ref[h] = acc_ref[h] * shrink + acc

    ahead = [scores_of(h) for h in range(2)]
    waiting = None
    for h in range(heads):
        scores = ahead.pop(0)
        if h + 2 < heads:
            ahead.append(scores_of(h + 2))
        if diag:
            scores = jnp.where(keep, scores, -jnp.inf)
        top = jnp.max(scores, axis=0, keepdims=True)
        shrink = None
        if not first:
            old = top_ref[h]
            top = jnp.maximum(old, top)
            shrink = jnp.exp2(old - top)
        weights = jnp.exp2(scores - top).astype(jnp.bfloat16)
        if waiting:
            settle(*waiting)
        waiting = (h, weights, top, shrink)
    settle(*waiting)


def sds(shape, dtype):
    return jax.ShapeDtypeStruct(shape, dtype)


def turned(queries_ref, out_ref):
    for h in range(out_ref.shape[0]):
        out_ref[h] = queries_ref[:, h * HD : (h + 1) * HD].T


def open_state(where, queries, others, own):
    rows, width = queries.shape
    heads = width // HD

    def kernel(where_ref, queries_ref, others_ref, own_ref, *state):
        live = [r.at[:heads] for r in state]
        rest = [r.at[heads:] for r in state]
        turned(queries_ref, live[0])
        turned(others_ref, rest[0])
        absorb([own_ref], live, first=True, diag=True)

        @pl.when(where_ref[1] == 0)
        def _():
            absorb([own_ref], rest, first=True)

        @pl.when(where_ref[1] != 0)
        def _():
            rest[1][...] = jnp.full(rest[1].shape, LOWEST, jnp.float32)
            rest[2][...] = jnp.zeros(rest[2].shape, jnp.float32)
            rest[3][...] = jnp.zeros(rest[3].shape, jnp.float32)

    return pl.pallas_call(
        kernel,
        out_shape=(
            sds((2 * heads, HD, rows), jnp.bfloat16),
            sds((2 * heads, 1, rows), jnp.float32),
            sds((2 * heads, 1, rows), jnp.float32),
            sds((2 * heads, HD, rows), jnp.float32),
        ),
        in_specs=[SMEM, VMEM, VMEM, VMEM],
        out_specs=(VMEM,) * 4,
        compiler_params=params(),
        cost_estimate=cost(rows, rows, 2 * heads),
        name="open_state",
    )(where, queries, others, own)


def fold(where, state, ahead, behind, step, parting=False, heads=None):
    def kernel(where_ref, ahead_ref, behind_ref, *refs):
        live = refs[:4] if heads is None else [r.at[:heads] for r in refs[:4]]
        z = where_ref[0]
        size = where_ref[2]

        @pl.when(z + step >= size)
        def _():
            absorb([ahead_ref, behind_ref], live)

        @pl.when((z + step < size) & (z >= step))
        def _():
            def part(i, _):
                absorb([ahead_ref], [r.at[pl.ds(i * 4, 4)] for r in live])
                return 0

            lax.fori_loop(0, live[1].shape[0] // 4, part, 0)

        if parting:
            out_ref, stat_ref = refs[-2:]
            half = live[0].shape[0] // 2
            for h in range(half):
                total = live[2][half + h]
                scale = jnp.where(total > 0, 1.0 / jnp.where(total > 0, total, 1.0), 0.0)
                out_ref[h] = (live[3][half + h] * scale).astype(jnp.bfloat16)
                stat_ref[0, h] = live[1][half + h]
                stat_ref[1, h] = total

    full, _, rows = state[0].shape
    extra = (sds((full // 2, HD, rows), jnp.bfloat16), sds((2, full // 2, 1, rows), jnp.float32)) if parting else ()
    out = pl.pallas_call(
        kernel,
        out_shape=tuple(sds(a.shape, a.dtype) for a in state) + extra,
        in_specs=[SMEM] + [VMEM] * 6,
        out_specs=(VMEM,) * (4 + len(extra)),
        input_output_aliases={3 + i: i for i in range(4)},
        compiler_params=params(),
        cost_estimate=cost(2 * ahead.shape[1], rows, heads or full),
    )(where, ahead, behind, *state)
    return (out[:4], out[4:]) if parting else out


def join(where, state, parted, stats, ahead, step):
    heads, _, rows = parted.shape

    def kernel(where_ref, parted_ref, stats_ref, ahead_ref, *refs):
        state_in, state_out = refs[:4], refs[4:]
        live = (state_in[0].at[:heads],) + tuple(state_out)
        for h in range(heads):
            old, theirs = state_in[1][h], stats_ref[0, h]
            top = jnp.maximum(old, theirs)
            mine = jnp.exp2(old - top)
            part = jnp.exp2(theirs - top) * stats_ref[1, h]
            state_out[0][h] = top
            state_out[1][h] = state_in[2][h] * mine + part
            state_out[2][h] = state_in[3][h] * mine + parted_ref[h].astype(jnp.float32) * part

        @pl.when(where_ref[0] >= step)
        def _():
            absorb([ahead_ref], live)

    return pl.pallas_call(
        kernel,
        out_shape=tuple(sds((heads, *a.shape[1:]), a.dtype) for a in state[1:]),
        in_specs=[SMEM] + [VMEM] * 7,
        out_specs=(VMEM,) * 3,
        compiler_params=params(),
        cost_estimate=cost(ahead.shape[1], rows, heads),
        name="join",
    )(where, parted, stats, ahead, *state)


def column(where_ref, step, flip, width):
    y = lax.rem(where_ref[3] + step, SIDE)
    x = where_ref[4] if flip == 0 else 1 - where_ref[4]
    return pl.multiple_of((y * 2 + x) * width, width)


def project(att, weight_ref, start, width):
    return jnp.dot(att, weight_ref[:, pl.ds(start, width)], preferred_element_type=jnp.float32)


def close(where, state, ahead, step, out_weight, first, width):
    heads, _, rows = state[3].shape

    def kernel(where_ref, ahead_ref, q_ref, top_ref, sum_ref, acc_ref, weight_ref, att_ref, out_ref, *_):
        live = (q_ref.at[:heads], top_ref, sum_ref, acc_ref)

        @pl.when(where_ref[0] >= step)
        def _():
            absorb([ahead_ref], live)

        for h in range(heads):
            att_ref[:, h * HD : (h + 1) * HD] = (live[3][h] * (1.0 / live[2][h])).astype(jnp.bfloat16).T

        out_ref[:rows] = project(att_ref[...], weight_ref, column(where_ref, FAR, 1, width), width).astype(jnp.bfloat16)
        for i, d in enumerate(NEAR):
            terms = project(att_ref[:first], weight_ref, column(where_ref, d, 1, width), width)
            out_ref[rows + i * first : rows + (i + 1) * first] = terms.astype(jnp.bfloat16)

    att, out, *_ = pl.pallas_call(
        kernel,
        out_shape=(sds((rows, heads * HD), jnp.bfloat16), sds((rows + len(NEAR) * first, width), jnp.bfloat16))
        + tuple(sds(a.shape, a.dtype) for a in state[1:]),
        in_specs=[SMEM] + [VMEM] * 6,
        out_specs=(VMEM,) * 5,
        input_output_aliases={3: 2, 4: 3, 5: 4},
        compiler_params=params(),
        cost_estimate=cost(2 * rows, rows, heads),
        name="close",
    )(where, ahead, *state, out_weight)
    return att, out


def project_away(where, att, out_weight, first, width):
    rows = att.shape[0] - first

    def kernel(where_ref, att_ref, weight_ref, *outs):
        for out_ref, d in zip(outs, AWAY):
            for flip in range(2):
                terms = project(att_ref[first:], weight_ref, column(where_ref, d, flip, width), width)
                out_ref[flip] = terms.astype(jnp.bfloat16)

    return pl.pallas_call(
        kernel,
        out_shape=(sds((2, rows, width), jnp.bfloat16),) * len(AWAY),
        in_specs=[SMEM, VMEM, VMEM],
        out_specs=(VMEM,) * len(AWAY),
        compiler_params=params(),
        cost_estimate=cost(2 * rows, rows, 8),
        name="project_away",
    )(where, att, out_weight)


def project_here(where, att, out_weight, first, width):
    full = att.shape[0]
    rows = full - first

    def kernel(where_ref, att_ref, weight_ref, last_ref, first_ref):
        for flip in range(2):
            last_ref[flip] = project(att_ref[first:], weight_ref, column(where_ref, 0, flip, width), width)
        first_ref[:full] = project(att_ref[...], weight_ref, column(where_ref, FAR, 0, width), width)
        for i, d in enumerate(NEAR):
            terms = project(att_ref[:first], weight_ref, column(where_ref, d, 0, width), width)
            first_ref[full + i * first : full + (i + 1) * first] = terms

    return pl.pallas_call(
        kernel,
        out_shape=(sds((2, rows, width), jnp.float32), sds((full + len(NEAR) * first, width), jnp.float32)),
        in_specs=[SMEM, VMEM, VMEM],
        out_specs=(VMEM,) * 2,
        compiler_params=params(),
        cost_estimate=cost(2 * rows, rows, 8),
        name="project_here",
    )(where, att, out_weight)


def add_first(kept, got, first):
    total, width = kept.shape
    full = total - len(NEAR) * first

    def kernel(kept_ref, got_ref, here_ref, far_ref, *outs):
        far_ref[...] = (kept_ref[:full] + got_ref[:full].astype(jnp.float32)).astype(jnp.bfloat16)
        for i, out_ref in enumerate((here_ref, *outs)):
            here = slice(full + i * first, full + (i + 1) * first)
            out_ref[...] = (kept_ref[here] + got_ref[here].astype(jnp.float32)).astype(out_ref.dtype)

    near = sds((first, width), jnp.bfloat16)
    return pl.pallas_call(
        kernel,
        out_shape=(sds((first, width), jnp.float32), sds((full, width), jnp.bfloat16)) + (near,) * len(AWAY),
        in_specs=[VMEM] * 2,
        out_specs=(VMEM,) * (2 + len(AWAY)),
        compiler_params=params(),
        cost_estimate=pl.CostEstimate(flops=kept.size, bytes_accessed=8 * kept.size, transcendentals=0),
        name="add_first",
    )(kept, got)


def add_last(kept, got):
    _, rows, width = kept.shape

    def kernel(kept_ref, *refs):
        *got_refs, here_ref, out_ref = refs
        here_ref[...] = kept_ref[0] + sum(r[0].astype(jnp.float32) for r in got_refs)
        out_ref[...] = (kept_ref[1] + sum(r[1].astype(jnp.float32) for r in got_refs)).astype(jnp.bfloat16)

    return pl.pallas_call(
        kernel,
        out_shape=(sds((rows, width), jnp.float32), sds((rows, width), jnp.bfloat16)),
        in_specs=[VMEM] * (1 + len(got)),
        out_specs=(VMEM,) * 2,
        compiler_params=params(),
        cost_estimate=pl.CostEstimate(flops=kept.size, bytes_accessed=8 * kept.size, transcendentals=0),
        name="add_last",
    )(kept, *got)


def finish(first_here, first_got, far_got, last_here, last_got):
    rows, width = first_here.shape
    more = last_here.shape[0]

    def kernel(first_ref, *refs):
        *got_refs, far_ref, last_ref, swapped_ref, out_ref = refs
        far = far_ref[...].astype(jnp.float32)
        out_ref[:rows] = (first_ref[...] + far[:rows] + sum(r[...].astype(jnp.float32) for r in got_refs)).astype(jnp.bfloat16)
        out_ref[rows:] = (last_ref[...] + far[rows:] + swapped_ref[...].astype(jnp.float32)).astype(jnp.bfloat16)

    return pl.pallas_call(
        kernel,
        out_shape=sds((rows + more, width), jnp.bfloat16),
        in_specs=[VMEM] * (4 + len(first_got)),
        out_specs=VMEM,
        compiler_params=params(),
        name="finish",
    )(first_here, *first_got, far_got, last_here, last_got)


def steps(queries, keys, values, out_weight):
    chips = lax.axis_size("z")
    where = jnp.stack([lax.axis_index("z"), lax.axis_index("core"), jnp.int32(chips), lax.axis_index("y"), lax.axis_index("x")]).astype(jnp.int32)
    up = [(i, (i + 1) % chips) for i in range(chips)]
    down = [(i, (i - 1) % chips) for i in range(chips)]
    swap = lambda a: lax.ppermute(a, "core", [(0, 1), (1, 0)])
    own = jnp.stack([keys, values])
    others = swap(queries)
    half = chips // 2
    heads = queries.shape[1] // HD
    ahead, behind = [own], [own]
    for k in range(1, half + 1):
        ahead.append(lax.ppermute(ahead[-1], "z", up))
        if k < half:
            behind.append(lax.ppermute(behind[-1], "z", down))
    state = open_state(where, queries, others, own)
    for k in range(1, half - 1):
        state = fold(where, state, ahead[k], behind[k], k, k + 2 == half)
    state, (parted, stats) = state
    k = half - 1
    swap_ahead, swap_behind = swap(ahead[k]), swap(behind[k])
    parted, stats = swap(parted), swap(stats)
    state = fold(where, state, ahead[k], behind[k], k, heads=heads)
    state = fold(where, state, swap_ahead, swap_behind, k, heads=heads)
    last = swap(ahead[half])
    mine = join(where, state, parted, stats, ahead[half], half)
    width = out_weight.shape[1] // (2 * SIDE)
    first = queries.shape[0] * 4 // 16
    att, send = close(where, (state[0], *mine), last, half, out_weight, first, width)
    across = lambda a: lax.ppermute(a, "x", [(0, 1), (1, 0)])
    along = lambda a, d: lax.ppermute(a, "y", [(i, (i + d) % SIDE) for i in range(SIDE)])
    got_x = across(send)
    away = project_away(where, att, out_weight, first, width)
    got_y = [along(a, d) for a, d in zip(away, AWAY)]
    last_kept, first_kept = project_here(where, att, out_weight, first, width)
    first_here, far_away, *first_away = add_first(first_kept, got_x, first)
    far_got = along(far_away, FAR)
    first_got = [along(a, d) for a, d in zip(first_away, AWAY)]
    last_here, last_away = add_last(last_kept, got_y)
    last_got = across(last_away)
    return finish(first_here, first_got, far_got, last_here, last_got)


def solution(mesh):
    finer = Mesh(
        mesh.devices.reshape(mesh.shape["parts"], mesh.shape["context"] // 2, 2, SIDE, mesh.shape["tensor"] // SIDE),
        ("parts", "z", "core", "y", "x"),
    )
    in_specs = (
        P(PARTS_CONTEXT, TENSOR),
        P(PARTS_CONTEXT, TENSOR),
        P(PARTS_CONTEXT, TENSOR),
        P(TENSOR, None),
    )
    out_specs = P(PARTS_CONTEXT, TENSOR)
    return jax.shard_map(steps, mesh=finer, in_specs=in_specs, out_specs=out_specs, check_vma=False)
```
